256 devices in a mesh: dp: 8 (over z_lo, core), ep: 32 (over x, y, z_hi).
Axes of the slice: x: 4, y: 4, z: 8 (z_hi: 2, z_lo: 4; z = z_hi * 4 + z_lo), core: 2. Of those that a mesh axis runs over, the one named last changes fastest.
Arguments:
- tokens: bfloat16 [32768, 7168], P(('dp', 'ep')), may hold values from -6 to 6
- out_grad: bfloat16 [32768, 7168], P(('dp', 'ep')), may hold values from -3 to 3
- expert_ids: int32 [32768, 8], P(('dp', 'ep')), may hold values from 0 to 255, as said below
- route_weights: bfloat16 [32768, 8], P(('dp', 'ep')), may hold values from 0.099609375 to 1
- gate_matrix: bfloat16 [7168, 8192], P('dp', 'ep'), may hold values from -0.0625 to 0.0625
- up_matrix: bfloat16 [7168, 8192], P('dp', 'ep'), may hold values from -0.0625 to 0.0625
- down_matrix: bfloat16 [7168, 8192], P('dp', 'ep'), may hold values from -0.125 to 0.125
Outputs:
- input_gradient: bfloat16 [32768, 7168], P(('dp', 'ep'))
- route_gradient: float32 [32768, 8], P(('dp', 'ep'))
- gate_gradient: bfloat16 [7168, 8192], P('dp', 'ep')
- up_gradient: bfloat16 [7168, 8192], P('dp', 'ep')
- down_gradient: bfloat16 [7168, 8192], P('dp', 'ep')
The draws below stay inside these ranges and needn't reach their ends.
Inputs may be any that keep to these rules, and one draw needn't show every extreme that they name: `expert_ids`: each row names 8 different ids, 2 in each of 4 groups of 32 consecutive ids. In each aligned block of 4096 rows, one id that is a multiple of 64 is named by 8 or more rows of every aligned block of 128 rows inside it.
All inputs are finite; a program needn't handle non-finite values.
Results may differ from the reference program's by a relative error of at most 0.014.
Values may be sent and summed in bfloat16 or wider, within the bound.
No kernel may reach another device: no remote copies, remote signals or barrier semaphores. Data moves between devices by JAX's collectives and lax.ppermute only.
A program may use at most 128 MiB of HBM per device.

```python
import math
import jax
import jax.numpy as jnp
from jax import lax

D = 7168
FF = 2048
ROUTED = 256
NGROUPS = 8
TOPG = 4
TOPK = 8
SLICES = 8
TOK_DEV = 128
HID_DEV = 256
EXPERTS = 4
STRIDE = 64
CAP = 8
TOKENS = 32768
N_DP = 8
N_EP = 32


def draw_expert_ids(key, part):
    total_rows = TOK_DEV * N_EP * N_DP
    group_width = ROUTED // NGROUPS
    per_group = TOPK // TOPG
    base = jax.random.fold_in(key, 7)
    key_hot = jax.random.fold_in(base, 1)
    key_groups = jax.random.fold_in(base, 2)
    key_members = jax.random.fold_in(base, 3)
    hottest = jax.random.randint(key_hot, (N_DP,), 0, EXPERTS) * STRIDE
    row_index = jnp.arange(total_rows, dtype=jnp.int32)
    forced = row_index % TOK_DEV < CAP
    hot_expert = hottest[row_index // (TOK_DEV * N_EP)]
    hot_group = hot_expert // group_width
    group_index = jnp.arange(NGROUPS, dtype=jnp.int32)
    group_scores = jax.random.randint(key_groups, (total_rows, NGROUPS), 0, 4096) * NGROUPS + group_index[None, :]
    group_scores = group_scores + jnp.where(forced[:, None] & (group_index[None, :] == hot_group[:, None]), 1 << 24, 0)
    chosen_groups = lax.top_k(group_scores, TOPG)[1].astype(jnp.int32)
    member_index = jnp.arange(group_width, dtype=jnp.int32)
    candidates = chosen_groups[:, :, None] * group_width + member_index[None, None, :]
    member_scores = jax.random.randint(key_members, (total_rows, TOPG, group_width), 0, 4096) * group_width + member_index[None, None, :]
    member_scores = member_scores + jnp.where(forced[:, None, None] & (candidates == hot_expert[:, None, None]), 1 << 24, 0)
    picked = lax.top_k(member_scores, per_group)[1]
    chosen = jnp.take_along_axis(candidates, picked, axis=2)
    return chosen.reshape(total_rows, TOPK).astype(jnp.int32)


def levels(rng, extent, cuts, smallest, high):
    factor_of, own = 1.0, jax.random.fold_in(rng, 6)
    for axis_at, parts in cuts:
        steps = jnp.exp(jax.random.uniform(jax.random.fold_in(own, axis_at), (parts,), jnp.float32, smallest / len(cuts), high / len(cuts)))
        factor_of = factor_of * jnp.repeat(steps, extent[axis_at] // parts).reshape([-1 if axis == axis_at else 1 for axis in range(len(extent))])
    return factor_of


def noise(key, shape, spread, reach, shards=(), kind=jnp.bfloat16):
    values = spread * jax.random.normal(key, shape, jnp.float32)
    if shards:
        values = values * levels(key, shape, shards, -0.22, 0.18)
    return jnp.clip(values, -reach, reach).astype(kind)


def setup_inputs(seed: int = 0) -> dict:
    keys = jax.random.split(jax.random.key(seed), 8)
    return {
        "tokens": noise(keys[0], (TOKENS, D), 1.0, 6.0, ((0, 256),)),
        "out_grad": noise(keys[1], (TOKENS, D), 0.5, 3.0, ((0, 256),)),
        "expert_ids": draw_expert_ids(jax.random.fold_in(keys[7], 71), 0),
        "route_weights": jnp.clip(jnp.exp(math.log(1.0) - 2.306499 * jax.random.uniform(keys[3], (TOKENS, TOPK), jnp.float32) ** levels(keys[3], (TOKENS, TOPK), ((0, 256),), -0.2, 0.2)), 0.099609375, 1.0).astype(jnp.bfloat16),
        "gate_matrix": noise(keys[4], (D, EXPERTS * FF), D ** -0.5, 0.0625, ((0, 8), (1, 32))),
        "up_matrix": noise(keys[5], (D, EXPERTS * FF), D ** -0.5, 0.0625, ((0, 8), (1, 32))),
        "down_matrix": noise(keys[6], (D, EXPERTS * FF), FF ** -0.5, 0.125, ((0, 8), (1, 32))),
    }


def assignments(expert_ids):
    blocks = expert_ids.shape[0] // TOK_DEV
    flat_ids = expert_ids.reshape(blocks, TOK_DEV * TOPK)
    window = (flat_ids % STRIDE) == 0
    expert = jnp.where(window, flat_ids // STRIDE, EXPERTS).astype(jnp.int32)
    column = jnp.arange(EXPERTS, dtype=jnp.int32)
    onehot = (expert[:, :, None] == column[None, None, :]).astype(jnp.int32)
    earlier = jnp.cumsum(onehot, axis=1) - onehot
    slot_index = jnp.sum(earlier * onehot, axis=2)
    kept_entry = window & (slot_index < CAP)
    target = expert * CAP + slot_index
    places = jnp.arange(EXPERTS * CAP, dtype=jnp.int32)
    table = kept_entry[:, :, None] & (target[:, :, None] == places[None, None, :])
    return table.reshape(blocks, TOK_DEV, TOPK, EXPERTS * CAP).astype(jnp.float32)


def widen(values):
    return lax.optimization_barrier(values.astype(jnp.bfloat16)).astype(jnp.float32)


def reference(tokens, out_grad, expert_ids, route_weights, gate_matrix, up_matrix, down_matrix):
    table = assignments(expert_ids)
    blocks = table.shape[0]
    select = jnp.sum(table, axis=2)
    select_half = select.astype(jnp.bfloat16)

    def dispatch_block(arguments):
        choose, block_in, block_grad = arguments
        first = jnp.dot(choose.T, block_in, preferred_element_type=jnp.float32).astype(jnp.bfloat16)
        second = jnp.dot(choose.T, block_grad, preferred_element_type=jnp.float32).astype(jnp.bfloat16)
        return first, second

    slot_in, slot_grad = lax.map(dispatch_block, (select_half, tokens.reshape(blocks, TOK_DEV, D), out_grad.reshape(blocks, TOK_DEV, D)))
    slot_gate = jnp.einsum("btks,btk->bs", table, route_weights.astype(jnp.float32).reshape(blocks, TOK_DEV, TOPK), precision=lax.Precision.HIGHEST).astype(jnp.bfloat16)

    def arrange(values):
        shaped = values.reshape((N_DP, N_EP, EXPERTS, CAP) + values.shape[2:])
        moved = jnp.moveaxis(shaped, 2, 0)
        return moved.reshape((EXPERTS, N_DP, N_EP * CAP) + values.shape[2:])

    def unarrange(values):
        shaped = values.reshape((EXPERTS, N_DP, N_EP, CAP) + values.shape[3:])
        moved = jnp.moveaxis(shaped, 0, 2)
        return moved.reshape((blocks, EXPERTS * CAP) + values.shape[3:])

    def expert_backward(arguments):
        rows_in, rows_grad, rows_gate, expert = arguments
        begin = (expert * FF).astype(jnp.int32)
        gate_cols = lax.dynamic_slice_in_dim(gate_matrix, begin, FF, 1)
        up_cols = lax.dynamic_slice_in_dim(up_matrix, begin, FF, 1)
        down_cols = lax.dynamic_slice_in_dim(down_matrix, begin, FF, 1)

        def one_group(total, group_arguments):
            group_in, group_grad, group_gate = group_arguments
            row_count = group_in.shape[0]
            gate_pre = jnp.dot(group_in, gate_cols, preferred_element_type=jnp.float32)
            up_pre = jnp.dot(group_in, up_cols, preferred_element_type=jnp.float32)
            projected = jnp.dot(group_grad, down_cols, preferred_element_type=jnp.float32)
            sigmoid = jax.nn.sigmoid(gate_pre)
            swished = gate_pre * sigmoid
            hidden = widen(swished * up_pre)
            slice_sums = jnp.sum((hidden * projected).reshape(row_count, SLICES, HID_DEV), axis=2)
            route_part = jnp.sum(widen(slice_sums), axis=1)
            scaling = group_gate.astype(jnp.float32)[:, None]
            grad_hidden = scaling * projected
            gate_delta = (grad_hidden * up_pre * sigmoid * (1.0 + gate_pre * (1.0 - sigmoid))).astype(jnp.bfloat16)
            up_delta = (grad_hidden * swished).astype(jnp.bfloat16)
            scaled = (scaling * hidden).astype(jnp.bfloat16)
            partial_value = jnp.zeros((row_count, D), jnp.float32)
            for piece in range(SLICES):
                low = piece * HID_DEV
                high = low + HID_DEV
                term = jnp.dot(gate_delta[:, low:high], gate_cols[:, low:high].T, preferred_element_type=jnp.float32)
                term = term + jnp.dot(up_delta[:, low:high], up_cols[:, low:high].T, preferred_element_type=jnp.float32)
                partial_value = partial_value + widen(term)
            grads = jnp.concatenate([
                jnp.dot(group_in.T, gate_delta, preferred_element_type=jnp.float32),
                jnp.dot(group_in.T, up_delta, preferred_element_type=jnp.float32),
                jnp.dot(group_grad.T, scaled, preferred_element_type=jnp.float32)], axis=1)
            total = total + widen(grads)
            return total, (partial_value, route_part)

        start_total = jnp.zeros((D, 3 * FF), jnp.float32)
        total, outputs = lax.scan(one_group, start_total, (rows_in, rows_grad, rows_gate))
        return total.astype(jnp.bfloat16), outputs[0], outputs[1]

    totals, partials, route_parts = lax.map(expert_backward, (arrange(slot_in), arrange(slot_grad), arrange(slot_gate), jnp.arange(EXPERTS, dtype=jnp.int32)))
    slot_partial = unarrange(partials)
    slot_route = unarrange(route_parts)

    def combine_block(arguments):
        choose, values = arguments
        return jnp.dot(choose, values, precision=lax.Precision.HIGHEST).astype(jnp.bfloat16)

    input_gradient = lax.map(combine_block, (select, slot_partial)).reshape(blocks * TOK_DEV, D)
    route_gradient = jnp.einsum("btks,bs->btk", table, slot_route, precision=lax.Precision.HIGHEST).reshape(blocks * TOK_DEV, TOPK)
    gate_gradient = jnp.moveaxis(totals[:, :, :FF], 0, 1).reshape(D, EXPERTS * FF)
    up_gradient = jnp.moveaxis(totals[:, :, FF:2 * FF], 0, 1).reshape(D, EXPERTS * FF)
    down_gradient = jnp.moveaxis(totals[:, :, 2 * FF:], 0, 1).reshape(D, EXPERTS * FF)
    return (input_gradient, route_gradient, gate_gradient, up_gradient, down_gradient)
```

```python
import jax
import jax.numpy as jnp
from jax import lax
from jax.sharding import Mesh, PartitionSpec as P

ROUTED = 256
TOPK = 8
SLICES = 8
CAP = 8
PAIR = 2
LANES = 128

EVERY = ("dp", "x", "y", "zh")
ACROSS = ("dp", "x", "zh")


def routes(expert_ids, route_weights, experts):
    rows = expert_ids.shape[0]
    stride = ROUTED // experts
    flat_ids = expert_ids.reshape(rows * TOPK)
    window = flat_ids % stride == 0
    expert = jnp.where(window, flat_ids // stride, experts)
    column = jnp.arange(experts, dtype=jnp.int32)
    onehot = (expert[:, None] == column[None, :]).astype(jnp.int32)
    earlier = jnp.cumsum(onehot, axis=0) - onehot
    slot_index = jnp.sum(earlier * onehot, axis=1)
    kept_entry = window & (slot_index < CAP)
    places = jnp.arange(experts * CAP, dtype=jnp.int32)
    assign = kept_entry[:, None] & ((expert * CAP + slot_index)[:, None] == places[None, :])
    assign = assign.astype(jnp.float32).reshape(rows, TOPK, experts * CAP)
    select = jnp.sum(assign, axis=1)
    weights = route_weights.astype(jnp.float32)
    weighted = jnp.sum(assign * weights[:, :, None], axis=1)
    inverse = assign / weights[:, :, None]
    return select.astype(jnp.bfloat16), weighted.astype(jnp.bfloat16), inverse


def dispatch(choose, values, parts, experts):
    slots = jnp.einsum("ts,td->sd", choose, values, preferred_element_type=jnp.float32)
    slots = slots.astype(jnp.bfloat16).reshape(experts, CAP, parts, -1)
    slots = jnp.transpose(slots, (2, 0, 1, 3))[:, :, None]
    width = slots.shape[-1]
    send = jnp.broadcast_to(slots, (parts, experts, PAIR, CAP, width))
    send = send.reshape(parts * experts * PAIR, CAP, width)
    got = lax.all_to_all(send, ACROSS, split_axis=0, concat_axis=0, tiled=True)
    return lax.all_gather(got.reshape(-1, width), "y", axis=0, tiled=True)


def body(tokens, out_grad, expert_ids, route_weights, gate_matrix, up_matrix, down_matrix):
    parts = lax.axis_size("dp")
    experts = lax.axis_size("x")
    turns = lax.axis_size("y")
    width = gate_matrix.shape[0]
    hid = gate_matrix.shape[1]
    select, weighted, inverse = routes(expert_ids, route_weights, experts)
    rows_in = dispatch(select, tokens, parts, experts)
    rows_grad = dispatch(weighted, out_grad, parts, experts)
    total = rows_in.shape[0]
    pair = jnp.concatenate([gate_matrix, up_matrix], axis=1)
    first = jnp.dot(rows_in, pair, preferred_element_type=jnp.float32).astype(jnp.bfloat16)
    second = jnp.dot(rows_grad, down_matrix, preferred_element_type=jnp.float32).astype(
        jnp.bfloat16
    )
    gate_up = lax.psum_scatter(first, "dp", scatter_dimension=0, tiled=True)
    projected = lax.psum_scatter(second, "dp", scatter_dimension=0, tiled=True)
    gate_pre = gate_up[:, :hid].astype(jnp.float32)
    up_pre = gate_up[:, hid:].astype(jnp.float32)
    projected = projected.astype(jnp.float32)
    sigmoid = jax.nn.sigmoid(gate_pre)
    swished = gate_pre * sigmoid
    hidden = swished * up_pre
    route_part = jnp.sum(hidden * projected, axis=1)
    gate_delta = projected * up_pre * sigmoid * (1.0 + gate_pre * (1.0 - sigmoid))
    up_delta = projected * swished
    mine = jnp.concatenate([gate_delta, up_delta, hidden], axis=1).astype(jnp.bfloat16)
    every = lax.all_gather(mine, "dp", axis=0, tiled=True)
    deltas = every[:, : 2 * hid]
    hiddens = every[:, 2 * hid :]
    partial = jnp.einsum("rh,dh->rd", deltas, pair, preferred_element_type=jnp.float32)
    own = lax.axis_index("dp")
    spread = jnp.where(
        jnp.arange(parts, dtype=jnp.int32)[:, None] == own, route_part[None, :], 0.0
    ).reshape(total, 1)
    partial = jnp.concatenate(
        [partial.astype(jnp.bfloat16), jnp.broadcast_to(spread, (total, LANES)).astype(jnp.bfloat16)],
        axis=1,
    )
    summed = lax.psum_scatter(partial, "y", scatter_dimension=0, tiled=True)
    summed = summed.reshape(parts * experts * PAIR, CAP, width + LANES)
    back = lax.all_to_all(summed, ACROSS, split_axis=0, concat_axis=0, tiled=True)
    back = back.reshape(parts, experts, PAIR, CAP, width + LANES).astype(jnp.float32)
    back = jnp.sum(back, axis=2)
    slot_sums = jnp.transpose(back[..., :width], (1, 2, 0, 3)).reshape(
        experts * CAP, parts * width
    )
    route_sums = jnp.sum(back[..., width], axis=0).reshape(experts * CAP)
    input_gradient = jnp.dot(select.astype(jnp.float32), slot_sums).astype(jnp.bfloat16)
    route_gradient = jnp.einsum("tks,s->tk", inverse, route_sums)
    left = jnp.einsum("rd,rh->dh", rows_in, deltas, preferred_element_type=jnp.float32)
    left = left.astype(jnp.bfloat16)
    right = jnp.einsum("rd,rh->dh", rows_grad, hiddens, preferred_element_type=jnp.float32)
    right = right.astype(jnp.bfloat16)
    return (input_gradient, route_gradient, left[:, :hid], left[:, hid:], right)


def solution(mesh):
    parts, senders = mesh.devices.shape
    experts = senders // SLICES
    finer = Mesh(mesh.devices.reshape(parts, experts, SLICES // PAIR, PAIR), EVERY)
    rows = P(EVERY, None)
    tiles = P("dp", ("x", "y", "zh"))
    return jax.shard_map(
        body,
        mesh=finer,
        in_specs=(rows, rows, rows, rows, tiles, tiles, tiles),
        out_specs=(rows, rows, tiles, tiles, tiles),
        check_vma=False,
    )
```
